32 devices in a mesh: expert: 4 (over y, x), tensor: 4 (over z), replica: 2 (over core).
Axes of the slice: x: 2, y: 2, z: 4, core: 2. Of those that a mesh axis runs over, the one named last changes fastest.
Arguments:
- trained: float32 [4, 7168, 2048], P('replica', 'tensor', 'expert'), may hold values from -3080 to 3080
- snapshot: bfloat16 [4, 7168, 2048], P('replica', 'tensor', 'expert'), may hold values from -3072 to 3072
- changed: int32 [4, 56, 16], P('replica', 'tensor', 'expert'), may hold values from 0 to 1, as said below
- placement: int32 [4], replicated, may hold values from 0 to 3, each once
Outputs:
- rotated_update: bfloat16 [4, 7168, 2048], P('expert', None, 'tensor')
The draws below stay inside these ranges and needn't reach their ends.
Inputs may be any that keep to these rules, and one draw needn't show every extreme that they name: `placement`: each of the 4 experts appears exactly once. `changed`: in each aligned block of 14 block rows by 4 block columns of one expert, at most 32 entries are 1; for every expert some such block has exactly 32.
All inputs are finite; a program needn't handle non-finite values.
Results may differ from the reference program's by a relative error of at most 0.001.
Values may be sent and summed in bfloat16 or wider, within the bound.
No kernel may reach another device: no remote copies, remote signals or barrier semaphores. Data moves between devices by JAX's collectives and lax.ppermute only.
A program may use at most 64 MiB of HBM per device.

```python
import math
import jax
import jax.numpy as jnp
from jax import lax

D = 7168
FF = 2048
BLK = 128
E = 4
RB = 56
CB = 16
RBT = 14
CBE = 4
MOST = 32


def log_uniform(key, shape, low, high):
    return jnp.exp(jax.random.uniform(key, shape, jnp.float32, math.log(low), math.log(high)))


def draw_changed(key, part):
    tensor_groups = D // (BLK * RBT)
    expert_groups = FF // (BLK * CBE)
    group_count = tensor_groups * expert_groups
    block_count = RBT * CBE
    key_counts, key_forced, key_order = jax.random.split(jax.random.fold_in(key, 7), 3)
    counts = jax.random.randint(key_counts, (E, group_count), 0, MOST + 1)
    forced = jax.random.randint(key_forced, (E,), 0, group_count)
    counts = jnp.where(jnp.arange(group_count)[None, :] == forced[:, None], MOST, counts)
    scores = jax.random.randint(key_order, (E, group_count, block_count), 0, 1 << 16) * block_count
    scores = scores + jnp.arange(block_count, dtype=jnp.int32)[None, None, :]
    rank_ids = jnp.argsort(jnp.argsort(scores, axis=2), axis=2)
    chosen_mask = (rank_ids < counts[:, :, None]).astype(jnp.int32)
    chosen_mask = chosen_mask.reshape(E, tensor_groups, expert_groups, RBT, CBE)
    chosen_mask = jnp.transpose(chosen_mask, (0, 1, 3, 2, 4))
    return chosen_mask.reshape(E, tensor_groups * RBT, expert_groups * CBE)


def base_values(key):
    key_base = jax.random.fold_in(key, 11)
    return 512.0 * jnp.clip(jax.random.normal(key_base, (E, D, FF), jnp.float32), -6.0, 6.0)


def draw_snapshot(key, part):
    return base_values(key).astype(jnp.bfloat16)


def draw_trained(key, part):
    anchor = base_values(key).astype(jnp.bfloat16).astype(jnp.float32)
    block_flags = draw_changed(key, part)
    key_large, key_small, key_jitter = jax.random.split(jax.random.fold_in(key, 23), 3)
    large_scale = log_uniform(key_large, (E, RB, CB), 0.25, 1.0)
    jitter = jnp.clip(jax.random.normal(key_jitter, (E, D, FF), jnp.float32), -6.0, 6.0)
    small_scale = log_uniform(key_small, (E, RB, CB), 0.04, 0.12)
    scales = jnp.where(block_flags == 1, large_scale, small_scale)
    jitter = jitter.reshape(E, RB, BLK, CB, BLK) * scales[:, :, None, :, None]
    return anchor + jitter.reshape(E, D, FF)


def setup_inputs(seed: int = 0) -> dict:
    key_of = jax.random.split(jax.random.key(seed), 5)
    return {
        "trained": draw_trained(jax.random.fold_in(key_of[4], 71), 0),
        "snapshot": draw_snapshot(jax.random.fold_in(key_of[4], 71), 0),
        "changed": draw_changed(jax.random.fold_in(key_of[4], 71), 0),
        "placement": jax.random.permutation(key_of[3], E).astype(jnp.int32),
    }


def hadamard():
    positions = jnp.arange(BLK, dtype=jnp.int32)
    parity = jnp.zeros((BLK, BLK), jnp.int32)
    for bit_level in range(BLK.bit_length() - 1):
        parity = parity + (positions[:, None] >> bit_level & 1) * (positions[None, :] >> bit_level & 1)
    return (1 - 2 * (parity % 2)).astype(jnp.float32) / math.sqrt(BLK)

def reference(trained, snapshot, changed, placement):
    hadamard_table = hadamard()

    def one_slot(expert):
        newest = trained[expert]
        previous = snapshot[expert].astype(jnp.float32)
        block_flags = changed[expert]
        delta_grid = (newest - previous).reshape(RB, BLK, CB, BLK)
        delta_grid = jnp.where(block_flags[:, None, :, None] == 1, delta_grid, 0.0).reshape(RB, BLK, FF)
        coded_grid = jnp.einsum('ij,ajc->aic', hadamard_table, delta_grid, precision=lax.Precision.HIGHEST)
        return coded_grid.reshape(D, FF).astype(jnp.bfloat16)
    return lax.map(one_slot, placement)
```

```python
import functools
import math

import jax
import jax.numpy as jnp
from jax import lax
from jax.experimental import pallas as pl
from jax.experimental.pallas import tpu as pltpu
from jax.sharding import PartitionSpec as P

BLK = 128
TAG_ROWS = 16
GROUP = 4


def encode_kernel(lo, hi, tagged, halves, flags, core, new_hbm, old_hbm, own, oth, spots, new, old, new_sem, old_sem):
    experts, block_count = flags.shape
    block_cols = new_hbm.shape[2] // BLK
    ranks = hi - lo
    part = BLK // halves

    def list_expert(p):
        def scan(b, found):
            spots[p, found] = b
            return found + flags[p, b]

        return lax.fori_loop(0, block_count, scan, jnp.int32(0))

    def copies(p, j):
        spot = spots[p, lo + j]
        rows = pl.ds(pl.multiple_of((spot // block_cols) * BLK, BLK), BLK)
        cols = pl.ds(pl.multiple_of((spot % block_cols) * BLK, BLK), BLK)
        lane = pl.ds(pl.multiple_of(j * BLK, BLK), BLK)
        return (
            pltpu.make_async_copy(new_hbm.at[p, rows, cols], new.at[p, :, lane], new_sem.at[p, j]),
            pltpu.make_async_copy(old_hbm.at[p, rows, cols], old.at[p, :, lane], old_sem.at[p, j]),
        )

    counts = []
    for p in range(experts):
        total = list_expert(p)
        count = jnp.clip(total - lo, 0, ranks)
        counts.append((total, count))

        @pl.loop(0, count)
        def _(j, p=p):
            for copy in copies(p, j):
                copy.start()

    row = lax.broadcasted_iota(jnp.int32, (BLK, 2 * BLK), 0)
    column = lax.broadcasted_iota(jnp.int32, (BLK, 2 * BLK), 1) % BLK
    common = row & column
    for shift in (4, 2, 1):
        common = common ^ (common >> shift)
    signs = (1 - 2 * (common & 1)).astype(jnp.float32).astype(jnp.bfloat16)
    first = core[0] == 0
    lanes = lax.broadcasted_iota(jnp.int32, (TAG_ROWS, BLK), 1)
    for p in range(experts):
        total, count = counts[p]
        if tagged:

            def tag(j, held, p=p):
                return jnp.where(lanes == j, spots[p, j], held)

            held = lax.fori_loop(0, total, tag, jnp.full((TAG_ROWS, BLK), -1, jnp.int32))
            held = held.astype(jnp.float32).astype(jnp.bfloat16)
            own[p, pl.ds(ranks * part, TAG_ROWS), :] = held
            oth[p, pl.ds(ranks * part, TAG_ROWS), :] = held

        @pl.loop(0, pl.cdiv(count, GROUP))
        def _(g, p=p, count=count):
            for k in range(GROUP):

                @pl.when(g * GROUP + k < count)
                def _(k=k):
                    for copy in copies(p, g * GROUP + k):
                        copy.wait()

            lane = pl.ds(pl.multiple_of(g * (GROUP * BLK), GROUP * BLK), GROUP * BLK)
            delta = new[p, :, lane] - old[p, :, lane].astype(jnp.float32)
            high = delta.astype(jnp.bfloat16)
            low = (delta - high.astype(jnp.float32)).astype(jnp.bfloat16)
            coded = jnp.dot(signs, jnp.concatenate([high, low], axis=0), preferred_element_type=jnp.float32)
            coded = (coded * (1.0 / math.sqrt(BLK))).astype(jnp.bfloat16)
            for k in range(GROUP):
                top = coded[:part, k * BLK : (k + 1) * BLK]
                bottom = coded[part:, k * BLK : (k + 1) * BLK]
                at = pl.ds(pl.multiple_of((g * GROUP + k) * part, part), part)
                own[p, at, :] = jnp.where(first, top, bottom)
                oth[p, at, :] = jnp.where(first, bottom, top)


def encode(trained, snapshot, flags, core, lo, hi, tagged, halves):
    experts, block_count = flags.shape
    ranks = -(-(hi - lo) // GROUP) * GROUP
    rows = (hi - lo) * (BLK // halves) + (TAG_ROWS if tagged else 0)
    if ranks != hi - lo:
        raise ValueError("ranks")
    out = jax.ShapeDtypeStruct((experts, rows, BLK), jnp.bfloat16)
    return pl.pallas_call(
        functools.partial(encode_kernel, lo, hi, tagged, halves),
        out_shape=(out, out),
        in_specs=[
            pl.BlockSpec(memory_space=pltpu.SMEM),
            pl.BlockSpec(memory_space=pltpu.SMEM),
            pl.BlockSpec(memory_space=pl.ANY),
            pl.BlockSpec(memory_space=pl.ANY),
        ],
        out_specs=[pl.BlockSpec(memory_space=pltpu.VMEM)] * 2,
        scratch_shapes=[
            pltpu.SMEM((experts, block_count + 1), jnp.int32),
            pltpu.VMEM((experts, BLK, ranks * BLK), jnp.float32),
            pltpu.VMEM((experts, BLK, ranks * BLK), jnp.bfloat16),
            pltpu.SemaphoreType.DMA((experts, ranks)),
            pltpu.SemaphoreType.DMA((experts, ranks)),
        ],
        compiler_params=pltpu.CompilerParams(vmem_limit_bytes=32 << 20),
        cost_estimate=pl.CostEstimate(flops=4_000_000_000, bytes_accessed=4_000_000, transcendentals=0),
        name="encode",
    )(flags, core, trained, snapshot)


def place_kernel(pieces, ranks, lo, clear, block_cols, where, tags, *refs):
    mine, theirs = refs[:pieces], refs[pieces : 2 * pieces]
    refs = refs[2 * pieces + (0 if clear else 1) :]
    out, sems = refs[0], refs[1]
    if clear:
        zeros, zero_sem = refs[2], refs[3]
        zeros[...] = jnp.zeros_like(zeros)
        step = zeros.shape[0]

        def blank(i):
            return pltpu.make_async_copy(zeros, out.at[0, pl.ds(pl.multiple_of(i * step, step), step), :], zero_sem.at[i])

        @pl.loop(0, out.shape[1] // step)
        def _(i):
            blank(i).start()

        @pl.loop(0, out.shape[1] // step)
        def _(i):
            blank(i).wait()

    part = BLK // 2
    own_row = where[pieces, 0]

    def copies(i, j):
        spot = tags[i, lo + j]
        row = where[i, 0] + (spot // block_cols) * BLK
        cols = pl.ds(pl.multiple_of(where[i, 1] + (spot % block_cols) * BLK, BLK), BLK)
        source = pl.ds(pl.multiple_of(j * part, part), part)
        return [
            pltpu.make_async_copy(
                held.at[source, :],
                out.at[0, pl.ds(pl.multiple_of(row + start, part), part), cols],
                sems.at[k, i, j],
            )
            for k, (held, start) in enumerate(((mine[i], own_row), (theirs[i], part - own_row)))
        ]

    for turn in ("start", "wait"):
        for i in range(pieces):

            @pl.loop(0, ranks)
            def _(j, i=i, turn=turn):
                @pl.when(tags[i, lo + j] >= 0)
                def _():
                    for copy in copies(i, j):
                        getattr(copy, turn)()


def place(out, out_shape, mine, theirs, where, tags, lo, ranks, block_cols):
    pieces, clear = len(mine), out is None
    any_space = pl.BlockSpec(memory_space=pl.ANY)
    scratch = [pltpu.SemaphoreType.DMA((2, pieces, ranks))]
    if clear:
        rows = 256
        scratch += [
            pltpu.VMEM((rows, out_shape[2]), jnp.bfloat16),
            pltpu.SemaphoreType.DMA((out_shape[1] // rows,)),
        ]
    return pl.pallas_call(
        functools.partial(place_kernel, pieces, ranks, lo, clear, block_cols),
        out_shape=jax.ShapeDtypeStruct(out_shape, jnp.bfloat16),
        in_specs=[pl.BlockSpec(memory_space=pltpu.SMEM)] * 2
        + [pl.BlockSpec(memory_space=pltpu.VMEM)] * (2 * pieces)
        + ([] if clear else [any_space]),
        out_specs=any_space,
        scratch_shapes=scratch,
        input_output_aliases={} if clear else {2 + 2 * pieces: 0},
        compiler_params=pltpu.CompilerParams(vmem_limit_bytes=32 << 20),
        cost_estimate=pl.CostEstimate(flops=2_000_000_000, bytes_accessed=4_000_000, transcendentals=0),
        name="place",
    )(where, tags, *mine, *theirs, *([] if clear else [out]))


def body(trained, snapshot, changed, placement):
    local_experts, local_rows, local_cols = trained.shape
    copies = lax.axis_size("replica")
    tensor_count = lax.axis_size("tensor")
    expert_count = lax.axis_size("expert")
    members = expert_count // tensor_count
    block_rows, block_cols = local_rows // BLK, local_cols // BLK
    block_count = block_rows * block_cols
    capacity = (4 * block_count + 3) // 7
    axes = ("expert", "tensor", "replica")
    core, tensor, expert = (lax.axis_index(a).astype(jnp.int32) for a in ("replica", "tensor", "expert"))

    def device(e, t, r):
        return (e * tensor_count + t) * copies + r

    def permute(array, target):
        pairs = [
            (device(e, t, r), device(*target(e, t, r)))
            for e in range(expert_count)
            for t in range(tensor_count)
            for r in range(copies)
        ]
        return lax.ppermute(array, axes, pairs)

    flags = changed.reshape(local_experts, block_count)
    order = list(range(expert_count))
    half = len(order) // 2
    order = [m for pair in zip(order[:half], order[half:]) for m in pair]
    unit = max(GROUP, capacity // 2 // GROUP * GROUP)
    rounds = [(lo, min(lo + unit, capacity)) for lo in range(0, capacity, unit)]

    slots = [expert ^ (tensor * members) ^ m for m in order]
    chosen = [jnp.take(placement, s, axis=0) for s in slots]
    sources = [tensor ^ ((expert ^ m) // members) for m in order]
    where = jnp.stack(
        [jnp.stack([t * local_rows, ((expert ^ m) % members) * local_cols]) for m, t in zip(order, sources)]
        + [jnp.stack([core * (BLK // copies), core * 0])]
    ).astype(jnp.int32)

    out_shape = (1, tensor_count * local_rows, members * local_cols)
    out = tags = None
    for index, (lo, hi) in enumerate(rounds):
        own, oth = encode(trained, snapshot, flags, core[None], lo, hi, index == 0, copies)
        got = permute(oth, lambda e, t, r: (e, t, 1 - r))
        mine, theirs = [], []
        for m, g in zip(order, chosen):
            at = g % local_experts
            piece = jnp.where(
                g // local_experts == core,
                lax.dynamic_index_in_dim(own, at, 0, keepdims=False),
                lax.dynamic_index_in_dim(got, at, 0, keepdims=False),
            )
            piece = permute(piece, lambda e, t, r: (e ^ (t * members) ^ m, t, r))
            piece = permute(piece, lambda e, t, r: (e, (e ^ (t * members) ^ m) // members, r))
            mine.append(piece)
            theirs.append(permute(piece, lambda e, t, r: (e, t, 1 - r)))
        if index == 0:
            row = (hi - lo) * (BLK // copies)
            tags = jnp.stack([piece[row] for piece in mine]).astype(jnp.int32)
        out = place(out, out_shape, mine, theirs, where, tags, lo, hi - lo, block_cols)
    return out


def solution(mesh):
    split = P("replica", "tensor", "expert")
    return jax.shard_map(
        body,
        mesh=mesh,
        in_specs=(split, split, split, P()),
        out_specs=P("expert", None, "tensor"),
        check_vma=False,
    )
```

```python
import functools
import math

import jax
import jax.numpy as jnp
from jax import lax
from jax.experimental import pallas as pl
from jax.experimental.pallas import tpu as pltpu
from jax.sharding import PartitionSpec as P

BLK = 128
TAG_ROWS = 16
SMEM = pl.BlockSpec(memory_space=pltpu.SMEM)
VMEM = pl.BlockSpec(memory_space=pltpu.VMEM)
HBM = pl.BlockSpec(memory_space=pltpu.MemorySpace.HBM)


def axis(name):
    return lax.axis_index(name).astype(jnp.int32)


def params(mib):
    return pltpu.CompilerParams(vmem_limit_bytes=mib << 20)


def cost(flops, moved):
    return pl.CostEstimate(flops=flops, bytes_accessed=moved, transcendentals=0)


def encode_kernel(rounds, halves, flags, new_hbm, old_hbm, *refs):
    outs, (spots, new, old, new_sem, old_sem) = refs[: 2 * len(rounds)], refs[2 * len(rounds) :]
    experts, block_cols, block_rows = flags.shape
    part = BLK // halves

    def scan(a, found):
        found = list(found)
        for c in range(block_cols):
            for p in range(experts):
                spots[p, found[p]] = a * block_cols + c
                found[p] = found[p] + flags[p, c, a]
        return tuple(found)

    totals = lax.fori_loop(0, block_rows, scan, (jnp.int32(0),) * experts, unroll=2)

    def bounds(p, lo, hi):
        return jnp.minimum(lo, totals[p]), jnp.minimum(hi, totals[p])

    def sides(p, j):
        lane = pl.ds(pl.multiple_of(j * BLK, BLK), BLK)
        return (
            (new_hbm, new.at[p, :, lane], new_sem.at[p, j]),
            (old_hbm, old.at[p, :, lane], old_sem.at[p, j]),
        )

    for lo, hi in rounds:
        for p in range(experts):

            @pl.loop(*bounds(p, lo, hi))
            def _(j, p=p):
                spot = spots[p, j]
                rows = pl.ds(pl.multiple_of((spot // block_cols) * BLK, BLK), BLK)
                cols = pl.ds(pl.multiple_of((spot % block_cols) * BLK, BLK), BLK)
                for source, target, sem in sides(p, j):
                    pltpu.make_async_copy(source.at[p, rows, cols], target, sem).start()

    row = lax.broadcasted_iota(jnp.int32, (BLK, 2 * BLK), 0)
    column = lax.broadcasted_iota(jnp.int32, (BLK, 2 * BLK), 1) % BLK
    common = row & column
    for shift in (4, 2, 1):
        common = common ^ (common >> shift)
    signs = (1 - 2 * (common & 1)).astype(jnp.float32).astype(jnp.bfloat16)
    first = axis("replica") == 0
    lanes = lax.broadcasted_iota(jnp.int32, (TAG_ROWS, BLK), 1)
    for p in range(experts):

        def tag(j, held, p=p):
            return jnp.where(lanes == j, spots[p, j], held)

        held = lax.fori_loop(0, totals[p], tag, jnp.where(lanes == BLK - 1, totals[p], -1))
        held = held.astype(jnp.float32).astype(jnp.bfloat16)
        for out in outs[:2]:
            out[p, pl.ds((rounds[0][1] - rounds[0][0]) * part, TAG_ROWS), :] = held

    for i, (lo, hi) in enumerate(rounds):
        own, oth = outs[2 * i : 2 * i + 2]
        for p in range(experts):

            @pl.loop(*bounds(p, lo, hi))
            def _(j, p=p):
                for source, target, sem in sides(p, j):
                    pltpu.make_async_copy(source.at[p, pl.ds(0, BLK), pl.ds(0, BLK)], target, sem).wait()

        for p in range(experts):
            delta = new[p, :, lo * BLK : hi * BLK] - old[p, :, lo * BLK : hi * BLK].astype(jnp.float32)
            high = delta.astype(jnp.bfloat16)
            low = (delta - high.astype(jnp.float32)).astype(jnp.bfloat16)
            coded = jnp.dot(signs, jnp.concatenate([high, low], axis=0), preferred_element_type=jnp.float32)
            coded = (coded * (1.0 / math.sqrt(BLK))).astype(jnp.bfloat16)
            for k in range(hi - lo):
                top = coded[:part, k * BLK : (k + 1) * BLK]
                bottom = coded[part:, k * BLK : (k + 1) * BLK]
                own[p, k * part : (k + 1) * part, :] = jnp.where(first, top, bottom)
                oth[p, k * part : (k + 1) * part, :] = jnp.where(first, bottom, top)


def encode(trained, snapshot, flags, rounds, halves):
    experts, block_cols, block_rows = flags.shape
    ranks = rounds[-1][1]
    outs = []
    for i, (lo, hi) in enumerate(rounds):
        rows = (hi - lo) * (BLK // halves) + (0 if i else TAG_ROWS)
        outs += [jax.ShapeDtypeStruct((experts, rows, BLK), jnp.bfloat16)] * 2
    space = pltpu.MemorySpace.HBM
    return pl.pallas_call(
        functools.partial(encode_kernel, rounds, halves),
        out_shape=outs,
        in_specs=[SMEM, HBM, HBM],
        out_specs=[VMEM] * len(outs),
        scratch_shapes=[
            pltpu.SMEM((experts, block_cols * block_rows + 1), jnp.int32),
            pltpu.VMEM((experts, BLK, ranks * BLK), jnp.float32),
            pltpu.VMEM((experts, BLK, ranks * BLK), jnp.bfloat16),
            pltpu.SemaphoreType.DMA((experts, ranks)),
            pltpu.SemaphoreType.DMA((experts, ranks)),
        ],
        compiler_params=params(24),
        cost_estimate=cost(4_000_000_000, 4_000_000),
        name="encode",
    )(
        flags,
        pltpu.with_memory_space_constraint(trained, space),
        pltpu.with_memory_space_constraint(snapshot, space),
    )


def by_slot_kernel(placement, own, got, *outs):
    experts = own.shape[0]
    core, expert = axis("replica"), axis("expert")
    for k, out in enumerate(outs):
        chosen = placement[expert ^ k]
        here, at = chosen // experts == core, chosen % experts

        @pl.when(here)
        def _(out=out, at=at):
            out[...] = own[at]

        @pl.when(jnp.logical_not(here))
        def _(out=out, at=at):
            out[...] = got[at]


def by_slot(placement, own, got, count):
    out = jax.ShapeDtypeStruct(own.shape[1:], own.dtype)
    return pl.pallas_call(
        by_slot_kernel,
        out_shape=(out,) * count,
        in_specs=[SMEM, VMEM, VMEM],
        out_specs=[VMEM] * count,
        compiler_params=params(16),
        cost_estimate=cost(1_000_000_000, 2_000_000),
        name="by_slot",
    )(placement, own, got)


def by_range_kernel(members, *refs):
    count = len(refs) * members // (members + 1)
    pieces, outs = refs[:count], refs[count:]
    rows = pieces[0].shape[0]
    shift = axis("expert") ^ (axis("tensor") * members)
    for case in range(count):

        @pl.when(shift == case)
        def _(case=case):
            for j, out in enumerate(outs):
                for u in range(members):
                    out[pl.ds(u * rows, rows), :] = pieces[case ^ (j * members + u)][...]


def by_range(pieces, members):
    rows, cols = pieces[0].shape
    out = jax.ShapeDtypeStruct((members * rows, cols), pieces[0].dtype)
    return pl.pallas_call(
        functools.partial(by_range_kernel, members),
        out_shape=(out,) * (len(pieces) // members),
        in_specs=[VMEM] * len(pieces),
        out_specs=[VMEM] * (len(pieces) // members),
        compiler_params=params(16),
        cost_estimate=cost(1_000_000_000, 2_000_000),
        name="by_range",
    )(*pieces)


def clear_kernel(out, zeros, sems):
    zeros[...] = jnp.zeros_like(zeros)
    step = zeros.shape[0]

    def blank(i):
        return pltpu.make_async_copy(zeros, out.at[0, pl.ds(i * step, step), :], sems.at[i])

    for i in range(out.shape[1] // step):
        blank(i).start()
    for i in range(out.shape[1] // step):
        blank(i).wait()


def clear(shape, step):
    return pl.pallas_call(
        clear_kernel,
        out_shape=jax.ShapeDtypeStruct(shape, jnp.bfloat16),
        out_specs=HBM,
        scratch_shapes=[pltpu.VMEM((step, shape[2]), jnp.bfloat16), pltpu.SemaphoreType.DMA((shape[1] // step,))],
        compiler_params=params(4),
        cost_estimate=cost(2_000_000_000, 7_000_000),
        name="clear",
    )()


def place_kernel(turns, members, lo, ranks, block_cols, local_rows, local_cols, tags, *refs):
    count = len(turns)
    mine, theirs = refs[:count], refs[count : 2 * count]
    out, sems = refs[-2:]
    part = BLK // 2
    rows_each = mine[0].shape[0] // members
    own_row = axis("replica") * part
    tensor = axis("tensor")
    spans = []
    for i, turn in enumerate(turns):
        for u in range(members):
            line = turn * members + u
            found = jnp.clip(tags[line, BLK - 1] - lo, 0, ranks)
            spans.append((i, u, found))

            @pl.loop(0, found)
            def _(j, i=i, u=u, turn=turn, line=line):
                spot = tags[line, lo + j]
                row = (tensor ^ turn) * local_rows + (spot // block_cols) * BLK
                cols = pl.ds(pl.multiple_of(u * local_cols + (spot % block_cols) * BLK, BLK), BLK)
                source = pl.ds(pl.multiple_of(u * rows_each + j * part, TAG_ROWS), part)
                for k, (held, start) in enumerate(((mine[i], own_row), (theirs[i], part - own_row))):
                    target = out.at[0, pl.ds(pl.multiple_of(row + start, part), part), cols]
                    pltpu.make_async_copy(held.at[source, :], target, sems.at[k, i * members + u, j]).start()

    for i, u, found in spans:

        @pl.loop(0, found)
        def _(j, i=i, u=u):
            for k, held in enumerate((mine[i], theirs[i])):
                target = out.at[0, pl.ds(0, part), pl.ds(0, BLK)]
                pltpu.make_async_copy(held.at[pl.ds(0, part), :], target, sems.at[k, i * members + u, j]).wait()


def place(out, tags, mine, theirs, turns, members, lo, ranks, block_cols, local_rows, local_cols):
    count = len(turns)
    return pl.pallas_call(
        functools.partial(place_kernel, turns, members, lo, ranks, block_cols, local_rows, local_cols),
        out_shape=jax.ShapeDtypeStruct(out.shape, out.dtype),
        in_specs=[SMEM] + [VMEM] * (2 * count) + [HBM],
        out_specs=HBM,
        scratch_shapes=[pltpu.SemaphoreType.DMA((2, count * members, ranks))],
        input_output_aliases={1 + 2 * count: 0},
        compiler_params=params(16),
        cost_estimate=cost(2_000_000_000, 4_000_000),
        name="place",
    )(tags, *mine, *theirs, out)


def push(trained, snapshot, changed, placement):
    _, local_rows, local_cols = trained.shape
    copies = lax.axis_size("replica")
    tensor_count = lax.axis_size("tensor")
    expert_count = lax.axis_size("expert")
    members = expert_count // tensor_count
    block_rows, block_cols = local_rows // BLK, local_cols // BLK
    block_count = block_rows * block_cols
    capacity = (4 * block_count + 3) // 7
    axes = ("expert", "tensor", "replica")

    def device(e, t, r):
        return (e * tensor_count + t) * copies + r

    def permute(array, target):
        pairs = [
            (device(e, t, r), device(*target(e, t, r)))
            for e in range(expert_count)
            for t in range(tensor_count)
            for r in range(copies)
        ]
        return lax.ppermute(array, axes, pairs)

    def swap(e, t, r):
        return e, t, 1 - r

    flags = jnp.transpose(changed, (0, 2, 1))
    first = max(1, capacity * 3 // 8)
    rounds = [(0, first), (first, capacity)]
    far = [j for j in range(tensor_count) if j > 1]
    coded = encode(trained, snapshot, flags, rounds, copies)
    swapped = [permute(coded[2 * i + 1], swap) for i in range(len(rounds))]
    out = clear((1, tensor_count * local_rows, members * local_cols), 256)
    tags = None
    for i, (lo, hi) in enumerate(rounds):
        pieces = list(by_slot(placement, coded[2 * i], swapped[i], expert_count))
        for k in range(1, expert_count):
            pieces[k] = permute(pieces[k], lambda e, t, r: (e ^ k, t, r))
        pieces = list(by_range(pieces, members))
        for j in far + [1]:
            pieces[j] = permute(pieces[j], lambda e, t, r: (e, t ^ j, r))
        theirs = [permute(piece, swap) for piece in pieces]
        if i == 0:
            rows_each = pieces[0].shape[0] // members
            lines = [piece[u * rows_each + (hi - lo) * (BLK // copies)] for piece in pieces for u in range(members)]
            tags = jnp.stack(lines).astype(jnp.int32)
        groups = [[0, 1] + far] if i == 0 else [[0, 1]] + [[j] for j in far[::-1]]
        for group in groups:
            out = place(
                out,
                tags,
                [pieces[j] for j in group],
                [theirs[j] for j in group],
                group,
                members,
                lo,
                hi - lo,
                block_cols,
                local_rows,
                local_cols,
            )
    return out


def solution(mesh):
    split = P("replica", "tensor", "expert")
    return jax.shard_map(
        push,
        mesh=mesh,
        in_specs=(split, split, split, P()),
        out_specs=P("expert", None, "tensor"),
        check_vma=False,
    )
```

```python
import functools
import math

import jax
import jax.numpy as jnp
from jax import lax
from jax.experimental import pallas as pl
from jax.experimental.pallas import tpu as pltpu
from jax.sharding import PartitionSpec as P

BLK = 128
TAG_ROWS = 16
SMEM = pl.BlockSpec(memory_space=pltpu.SMEM)
VMEM = pl.BlockSpec(memory_space=pltpu.VMEM)
HBM = pl.BlockSpec(memory_space=pltpu.MemorySpace.HBM)


def axis(name):
    return lax.axis_index(name).astype(jnp.int32)


def params(mib):
    return pltpu.CompilerParams(vmem_limit_bytes=mib << 20)


def cost(flops, moved):
    return pl.CostEstimate(flops=flops, bytes_accessed=moved, transcendentals=0)


def encode_kernel(lo, hi, tagged, halves, flags_hbm, new_hbm, old_hbm, own, oth, flags, spots, new, old, flag_sem, new_sem, old_sem):
    copy = pltpu.make_async_copy(flags_hbm, flags, flag_sem)
    copy.start()
    experts, block_cols, block_rows = flags.shape
    part = BLK // halves
    row = lax.broadcasted_iota(jnp.int32, (BLK, 2 * BLK), 0)
    column = lax.broadcasted_iota(jnp.int32, (BLK, 2 * BLK), 1) % BLK
    common = row & column
    for shift in (4, 2, 1):
        common = common ^ (common >> shift)
    signs = (1 - 2 * (common & 1)).astype(jnp.float32).astype(jnp.bfloat16)
    first = axis("replica") == 0
    lanes = lax.broadcasted_iota(jnp.int32, (TAG_ROWS, BLK), 1)
    copy.wait()

    def scan(a, found):
        found = list(found)
        for c in range(block_cols):
            for p in range(experts):
                spots[p, found[p]] = a * block_cols + c
                found[p] = found[p] + flags[p, c, a]
        return tuple(found)

    totals = lax.fori_loop(0, block_rows, scan, (jnp.int32(0),) * experts, unroll=2)
    counts = [jnp.clip(total - lo, 0, hi - lo) for total in totals]

    def sides(p, j):
        lane = pl.ds(pl.multiple_of(j * BLK, BLK), BLK)
        return (
            (new_hbm, new.at[p, :, lane], new_sem.at[p, j]),
            (old_hbm, old.at[p, :, lane], old_sem.at[p, j]),
        )

    for p in range(experts):

        @pl.loop(0, counts[p])
        def _(j, p=p):
            spot = spots[p, lo + j]
            rows = pl.ds(pl.multiple_of((spot // block_cols) * BLK, BLK), BLK)
            cols = pl.ds(pl.multiple_of((spot % block_cols) * BLK, BLK), BLK)
            for source, target, sem in sides(p, j):
                pltpu.make_async_copy(source.at[p, rows, cols], target, sem).start()

    for p in range(experts if tagged else 0):

        def tag(j, held, p=p):
            return jnp.where(lanes == j, spots[p, j], held)

        held = lax.fori_loop(0, totals[p], tag, jnp.where(lanes == BLK - 1, totals[p], -1))
        held = held.astype(jnp.float32).astype(jnp.bfloat16)
        for out in (own, oth):
            out[p, pl.ds((hi - lo) * part, TAG_ROWS), :] = held

    for p in range(experts):

        @pl.loop(0, counts[p])
        def _(j, p=p):
            for source, target, sem in sides(p, j):
                pltpu.make_async_copy(source.at[p, pl.ds(0, BLK), pl.ds(0, BLK)], target, sem).wait()

        delta = new[p] - old[p].astype(jnp.float32)
        high = delta.astype(jnp.bfloat16)
        low = (delta - high.astype(jnp.float32)).astype(jnp.bfloat16)
        coded = jnp.dot(signs, jnp.concatenate([high, low], axis=0), preferred_element_type=jnp.float32)
        coded = (coded * (1.0 / math.sqrt(BLK))).astype(jnp.bfloat16)
        for k in range(hi - lo):
            top = coded[:part, k * BLK : (k + 1) * BLK]
            bottom = coded[part:, k * BLK : (k + 1) * BLK]
            own[p, k * part : (k + 1) * part, :] = jnp.where(first, top, bottom)
            oth[p, k * part : (k + 1) * part, :] = jnp.where(first, bottom, top)


def encode(trained, snapshot, flags, lo, hi, tagged, halves):
    experts, block_cols, block_rows = flags.shape
    ranks = hi - lo
    rows = ranks * (BLK // halves) + (TAG_ROWS if tagged else 0)
    out = jax.ShapeDtypeStruct((experts, rows, BLK), jnp.bfloat16)
    return pl.pallas_call(
        functools.partial(encode_kernel, lo, hi, tagged, halves),
        out_shape=(out, out),
        in_specs=[HBM] * 3,
        out_specs=[VMEM] * 2,
        scratch_shapes=[
            pltpu.SMEM(flags.shape, jnp.int32),
            pltpu.SMEM((experts, block_cols * block_rows + 1), jnp.int32),
            pltpu.VMEM((experts, BLK, ranks * BLK), jnp.float32),
            pltpu.VMEM((experts, BLK, ranks * BLK), jnp.bfloat16),
            pltpu.SemaphoreType.DMA,
            pltpu.SemaphoreType.DMA((experts, ranks)),
            pltpu.SemaphoreType.DMA((experts, ranks)),
        ],
        compiler_params=params(24),
        cost_estimate=cost(4_000_000_000, 4_000_000),
        name="encode",
    )(*(pltpu.with_memory_space_constraint(a, pltpu.MemorySpace.HBM) for a in (flags, trained, snapshot)))


def by_slot_kernel(placement, own, got, *outs):
    experts = own.shape[0]
    core, expert = axis("replica"), axis("expert")
    for k, out in enumerate(outs):
        chosen = placement[expert ^ k]
        here, at = chosen // experts == core, chosen % experts

        @pl.when(here)
        def _(out=out, at=at):
            out[...] = own[at]

        @pl.when(jnp.logical_not(here))
        def _(out=out, at=at):
            out[...] = got[at]


def by_slot(placement, own, got, count):
    out = jax.ShapeDtypeStruct(own.shape[1:], own.dtype)
    return pl.pallas_call(
        by_slot_kernel,
        out_shape=(out,) * count,
        in_specs=[SMEM, VMEM, VMEM],
        out_specs=[VMEM] * count,
        compiler_params=params(16),
        cost_estimate=cost(1_000_000_000, 2_000_000),
        name="by_slot",
    )(placement, own, got)


def by_range_kernel(members, count, held, *refs):
    pieces, kept, outs = refs[:count], refs[count : count + held], refs[count + held :]
    rows = pieces[0].shape[0]
    shift = axis("expert") ^ (axis("tensor") * members)
    for j in range(held):
        before = kept[j].shape[0] // members
        for u in range(members):
            outs[j][pl.ds(u * (before + rows), before), :] = kept[j][pl.ds(u * before, before), :]
    for case in range(count):

        @pl.when(shift == case)
        def _(case=case):
            for j, out in enumerate(outs):
                each = out.shape[0] // members
                for u in range(members):
                    out[pl.ds(u * each + each - rows, rows), :] = pieces[case ^ (j * members + u)][...]


def by_range(pieces, kept, members):
    rows, cols = pieces[0].shape
    total, count = len(pieces) // members, len(pieces)
    outs = []
    for j in range(total):
        before = kept[j].shape[0] if j < len(kept) else 0
        outs.append(jax.ShapeDtypeStruct((members * rows + before, cols), pieces[0].dtype))
    return pl.pallas_call(
        functools.partial(by_range_kernel, members, count, len(kept)),
        out_shape=outs,
        in_specs=[VMEM] * (count + len(kept)),
        out_specs=[VMEM] * total,
        compiler_params=params(16),
        cost_estimate=cost(1_000_000_000, 2_000_000),
        name="by_range",
    )(*pieces, *kept)


def clear_kernel(out, zeros, sems):
    zeros[...] = jnp.zeros_like(zeros)
    step = zeros.shape[0]

    def blank(i):
        return pltpu.make_async_copy(zeros, out.at[0, pl.ds(i * step, step), :], sems.at[i])

    for i in range(out.shape[1] // step):
        blank(i).start()
    for i in range(out.shape[1] // step):
        blank(i).wait()


def clear(shape, step):
    return pl.pallas_call(
        clear_kernel,
        out_shape=jax.ShapeDtypeStruct(shape, jnp.bfloat16),
        out_specs=HBM,
        scratch_shapes=[pltpu.VMEM((step, shape[2]), jnp.bfloat16), pltpu.SemaphoreType.DMA((shape[1] // step,))],
        compiler_params=params(4),
        cost_estimate=cost(2_000_000_000, 7_000_000),
        name="clear",
    )()


def place_kernel(turns, lines, members, lo, ranks, gap, block_cols, local_rows, local_cols, tags, *refs):
    count = len(turns)
    mine, theirs = refs[:count], refs[count : 2 * count]
    out, sems = refs[-2:]
    part = BLK // 2
    rows_each = mine[0].shape[0] // members
    own_row = axis("replica") * part
    tensor = axis("tensor")
    spans = []
    for i, turn in enumerate(turns):
        for u in range(members):
            line = lines[i] * members + u
            found = jnp.clip(tags[line, BLK - 1] - lo, 0, ranks)
            spans.append((i, u, found))

            @pl.loop(0, found)
            def _(j, i=i, u=u, turn=turn, line=line):
                spot = tags[line, lo + j]
                row = (tensor ^ turn) * local_rows + (spot // block_cols) * BLK
                cols = pl.ds(pl.multiple_of(u * local_cols + (spot % block_cols) * BLK, BLK), BLK)
                skip = jnp.where(j >= gap, TAG_ROWS, 0)
                source = pl.ds(pl.multiple_of(u * rows_each + j * part + skip, TAG_ROWS), part)
                for k, (held, start) in enumerate(((mine[i], own_row), (theirs[i], part - own_row))):
                    target = out.at[0, pl.ds(pl.multiple_of(row + start, part), part), cols]
                    pltpu.make_async_copy(held.at[source, :], target, sems.at[k, i * members + u, j]).start()

    for i, u, found in spans:

        @pl.loop(0, found)
        def _(j, i=i, u=u):
            for k, held in enumerate((mine[i], theirs[i])):
                target = out.at[0, pl.ds(0, part), pl.ds(0, BLK)]
                pltpu.make_async_copy(held.at[pl.ds(0, part), :], target, sems.at[k, i * members + u, j]).wait()


def place(out, tags, mine, theirs, turns, lines, members, lo, ranks, gap, sizes):
    count = len(turns)
    return pl.pallas_call(
        functools.partial(place_kernel, turns, lines, members, lo, ranks, gap, *sizes),
        out_shape=jax.ShapeDtypeStruct(out.shape, out.dtype),
        in_specs=[SMEM] + [VMEM] * (2 * count) + [HBM],
        out_specs=HBM,
        scratch_shapes=[pltpu.SemaphoreType.DMA((2, count * members, ranks))],
        input_output_aliases={1 + 2 * count: 0},
        compiler_params=params(16),
        cost_estimate=cost(2_000_000_000, 4_000_000),
        name="place",
    )(tags, *mine, *theirs, out)


def push(trained, snapshot, changed, placement):
    _, local_rows, local_cols = trained.shape
    copies = lax.axis_size("replica")
    tensor_count = lax.axis_size("tensor")
    expert_count = lax.axis_size("expert")
    members = expert_count // tensor_count
    block_rows, block_cols = local_rows // BLK, local_cols // BLK
    block_count = block_rows * block_cols
    capacity = (4 * block_count + 3) // 7
    axes = ("expert", "tensor", "replica")

    def device(e, t, r):
        return (e * tensor_count + t) * copies + r

    def permute(array, target):
        pairs = [
            (device(e, t, r), device(*target(e, t, r)))
            for e in range(expert_count)
            for t in range(tensor_count)
            for r in range(copies)
        ]
        return lax.ppermute(array, axes, pairs)

    def swap(e, t, r):
        return e, t, 1 - r

    flags = jnp.transpose(changed, (0, 2, 1))
    part = BLK // copies
    first = max(1, capacity * 3 // 8)
    rounds = [(0, first), (first, capacity)]
    near, far = [0], list(range(2, tensor_count)) + [1]
    sizes = (block_cols, local_rows, local_cols)
    out = clear((1, tensor_count * local_rows, members * local_cols), 256)

    def taken(pieces):
        lines = [p[u * (p.shape[0] // members) + first * part] for p in pieces for u in range(members)]
        return jnp.stack(lines).astype(jnp.int32)

    kept = []
    for i, (lo, hi) in enumerate(rounds):
        own, oth = encode(trained, snapshot, flags, lo, hi, i == 0, copies)
        got = permute(oth, swap)
        pieces = list(by_slot(placement, own, got, expert_count))
        for k in range(1, expert_count):
            pieces[k] = permute(pieces[k], lambda e, t, r: (e ^ k, t, r))
        pieces = list(by_range(pieces, kept, members))
        kept = pieces[: len(near)]
        for j in far:
            pieces[j] = permute(pieces[j], lambda e, t, r: (e, t ^ j, r))
        theirs = {j: permute(pieces[j], swap) for j in far}
        if i == 0:
            tags = taken([theirs[j] for j in sorted(far)])
        else:
            theirs.update({j: permute(kept[j], swap) for j in near})
            pair = [theirs[j] for j in near]
            out = place(out, taken(pair), kept, pair, near, near, members, 0, capacity, first, sizes)
        for group in [[j] for j in far[::-1]] if i else [sorted(far)]:
            out = place(
                out,
                tags,
                [pieces[j] for j in group],
                [theirs[j] for j in group],
                group,
                [j - len(near) for j in group],
                members,
                lo,
                hi - lo,
                hi - lo,
                sizes,
            )
    return out


def solution(mesh):
    split = P("replica", "tensor", "expert")
    return jax.shard_map(
        push,
        mesh=mesh,
        in_specs=(split, split, split, P()),
        out_specs=P("expert", None, "tensor"),
        check_vma=False,
    )
```
